32 devices in a mesh: ga: 8 (over y, x, core), ka: 4 (over z).
Axes of the slice: x: 2, y: 2, z: 4, core: 2. Of those that a mesh axis runs over, the one named last changes fastest.
Arguments:
- fine_waves: bfloat16 [64, 16, 40960], P('ka', None, 'ga'), may hold values from -6 to 6
- coarse_waves: bfloat16 [32, 16, 40960], P('ka', None, 'ga'), may hold values from -6 to 6
- coarse_kernel: bfloat16 [48, 64, 2048], P('ga', None, 'ka'), may hold values from -6 to 6
- row_valence: float32 [8, 8, 8, 8], P('ga'), may hold values from -6 to 6
- row_conduction: float32 [8, 8, 8, 8], P('ga'), may hold values from -6 to 6
- row_neighbours: int32 [8, 8], P('ga'), may hold values from 0 to 11, as said below
- row_weight_index: int32 [8, 8], P('ga'), may hold values from 0 to 7
- col_neighbours: int32 [64, 8], P('ka'), may hold values from 0 to 7, as said below
- col_weight_index: int32 [64, 8], P('ka'), may hold values from 0 to 7
- tile_list: int32 [4, 8], replicated, may hold values from 0 to 31, as said below
- weight_table: float32 [8], replicated, may hold values from 0.2 to 0.5
Outputs:
- fine_kernel: bfloat16 [8, 64, 4096], P('ga', 'ka')
The draws below stay inside these ranges and needn't reach their ends.
Inputs may be any that keep to these rules, and one draw needn't show every extreme that they name: `row_neighbours`: each row names 8 distinct positions; a position p below 6 is coarse row p of the fine row's own group r, a larger one is coarse row p - 6 of the next group (the last group's next is group 0); each row names three or more of each kind. `col_neighbours`: each fine column names 8 distinct positions of its owner's list, and every position of the list is named by some column of that owner. `tile_list`: row o lists 8 distinct coarse columns in rising order of their holder (column p is held by owner p // 8); no row takes more than 4 columns from one holder, and every row takes exactly 4 from some holder.
All inputs are finite; a program needn't handle non-finite values.
Results may differ from the reference program's by a relative error of at most 0.0064.
Values may be sent and summed in bfloat16 or wider, within the bound.
No kernel may reach another device: no remote copies, remote signals or barrier semaphores. Data moves between devices by JAX's collectives and lax.ppermute only.
A program may use at most 64 MiB of HBM per device.

```python
import math
import jax
import jax.numpy as jnp
from jax import lax

VALENCE = 8
CONDUCTION = 8
PLANE_WAVES = 40960
CORNERS = 8
BAND_PAIRS = 64
ROWS_DEVICE = 1
SLAB_ROWS = 8
GROUP_ROWS = 6
COARSE_ROWS = 48
OWNER_COLUMNS = 16
FINE_COLUMNS = 64
OWNER_COARSE = 8
COARSE_COLUMNS = 32
SLOT_COUNT = 4
LIST_LENGTH = 8
WEIGHT_LEVELS = 8
N_KA = 4


def draw_row_neighbours(key, part):
    row_keys = jax.random.split(key, SLAB_ROWS)

    def one_row(subkey):
        first_key, second_key, third_key = jax.random.split(subkey, 3)
        own_rows = jax.random.permutation(first_key, GROUP_ROWS)
        next_rows = jax.random.permutation(second_key, GROUP_ROWS) + GROUP_ROWS
        remaining = jnp.concatenate([own_rows[3:], next_rows[3:]])
        extra_rows = jax.random.permutation(third_key, remaining)[:2]
        return jnp.concatenate([own_rows[:3], next_rows[:3], extra_rows]).astype(jnp.int32)
    return jax.vmap(one_row)(row_keys)


def draw_col_neighbours(key, part):
    owner_key, column_key = jax.random.split(key)
    owner_keys = jax.random.split(owner_key, N_KA)
    covering = jax.vmap(lambda subkey: jax.random.permutation(subkey, LIST_LENGTH).reshape(LIST_LENGTH // CORNERS, CORNERS))(owner_keys)
    column_keys = jax.random.split(column_key, FINE_COLUMNS)
    picked = jax.vmap(lambda subkey: jax.random.permutation(subkey, LIST_LENGTH)[:CORNERS])(column_keys)
    picked = picked.reshape(N_KA, OWNER_COLUMNS, CORNERS)
    merged = picked.at[:, :LIST_LENGTH // CORNERS].set(covering)
    return merged.reshape(FINE_COLUMNS, CORNERS).astype(jnp.int32)


def draw_tile_list(key, part):
    owner_keys = jax.random.split(key, N_KA)

    def one_list(subkey):
        order_key, column_key = jax.random.split(subkey)
        holder_order = jax.random.permutation(order_key, N_KA)
        standing = jnp.zeros((N_KA,), jnp.int32).at[holder_order].set(jnp.arange(N_KA, dtype=jnp.int32))
        counts = jnp.where(standing < N_KA // 4, SLOT_COUNT, jnp.where(standing < N_KA // 2, 0, SLOT_COUNT // 2))
        column_keys = jax.random.split(column_key, N_KA)
        picked = jax.vmap(lambda inner: jax.random.permutation(inner, OWNER_COARSE)[:SLOT_COUNT])(column_keys)
        column_ids = picked + jnp.arange(N_KA, dtype=jnp.int32)[:, None] * OWNER_COARSE
        filled = jnp.arange(SLOT_COUNT, dtype=jnp.int32)[None, :] < counts[:, None]
        keep_order = jnp.argsort(jnp.where(filled, 0, 1).reshape(-1), stable=True)[:LIST_LENGTH]
        return column_ids.reshape(-1)[keep_order]
    return jax.vmap(one_list)(owner_keys).astype(jnp.int32)


def touch_ends(values, stream_key, least, top_value):
    spot = [jax.random.randint(jax.random.fold_in(stream_key, axis), (), 0, length) for axis, length in enumerate(values.shape)]
    main_axis = values.shape.index(max(values.shape))
    beside = spot[:main_axis] + [(spot[main_axis] + 1) % values.shape[main_axis]] + spot[main_axis + 1:]
    return values.at[tuple(spot)].set(least).at[tuple(beside)].set(top_value)


def level_of(stream_key, dims, shards, least, top_value):
    gain, own = 1.0, jax.random.fold_in(stream_key, 6)
    for dim, parts in shards:
        draws = jnp.exp(jax.random.uniform(jax.random.fold_in(own, dim), (parts,), jnp.float32, least / len(shards), top_value / len(shards)))
        gain = gain * jnp.repeat(draws, dims[dim] // parts).reshape([-1 if axis == dim else 1 for axis in range(len(dims))])
    return gain


def gaussian(own_key, shape, scale, bound, shards=(), kind=jnp.bfloat16):
    values = jax.random.normal(own_key, shape, jnp.float32) * scale
    if len(shards) > 0:
        values = level_of(own_key, shape, shards, -0.22, 0.18) * values
    return jnp.clip(values, min=-bound, max=bound).astype(kind)


def setup_inputs(seed: int = 0) -> dict:
    streams_of = jax.random.split(jax.random.key(seed), 12)
    return {
        "fine_waves": gaussian(streams_of[0], (FINE_COLUMNS, VALENCE + CONDUCTION, PLANE_WAVES), 1.0, 6.0, ((0, 4), (2, 8))),
        "coarse_waves": gaussian(streams_of[1], (COARSE_COLUMNS, VALENCE + CONDUCTION, PLANE_WAVES), 1.0, 6.0, ((0, 4), (2, 8))),
        "coarse_kernel": gaussian(streams_of[2], (COARSE_ROWS, BAND_PAIRS, COARSE_COLUMNS * BAND_PAIRS), 1.0, 6.0, ((0, 8), (2, 4))),
        "row_valence": gaussian(streams_of[3], (SLAB_ROWS, CORNERS, VALENCE, VALENCE), 1.0, 6.0, ((0, 8),), jnp.float32),
        "row_conduction": gaussian(streams_of[4], (SLAB_ROWS, CORNERS, CONDUCTION, CONDUCTION), 1.0, 6.0, ((0, 8),), jnp.float32),
        "row_neighbours": draw_row_neighbours(jax.random.fold_in(streams_of[11], 71), 0),
        "row_weight_index": touch_ends(jax.random.randint(streams_of[6], (SLAB_ROWS, CORNERS), 0, WEIGHT_LEVELS), jax.random.fold_in(streams_of[6], 1), 0, WEIGHT_LEVELS - 1).astype(jnp.int32),
        "col_neighbours": draw_col_neighbours(jax.random.fold_in(streams_of[11], 71), 0),
        "col_weight_index": touch_ends(jax.random.randint(streams_of[8], (FINE_COLUMNS, CORNERS), 0, WEIGHT_LEVELS), jax.random.fold_in(streams_of[8], 1), 0, WEIGHT_LEVELS - 1).astype(jnp.int32),
        "tile_list": draw_tile_list(jax.random.fold_in(streams_of[11], 71), 0),
        "weight_table": jnp.clip(jax.random.uniform(streams_of[10], (WEIGHT_LEVELS,), jnp.float32, 0.2, 0.5), 0.2, 0.5),
    }


def table_lookup(indices, weight_table):
    levels = jnp.arange(weight_table.shape[0], dtype=jnp.int32)
    return lax.optimization_barrier(jnp.sum(jnp.where(indices[..., None] == levels, weight_table, 0.0), axis=-1))

def rotation(weights, valence_part, conduction_part):
    outer_product = jnp.einsum('...vw,...xy->...vxwy', valence_part, conduction_part)
    tile_shape = outer_product.shape[:-4] + (BAND_PAIRS, BAND_PAIRS)
    scaled = weights[..., None, None] * outer_product.reshape(tile_shape) / math.sqrt(BAND_PAIRS)
    return scaled.astype(jnp.bfloat16)

def reference(fine_waves, coarse_waves, coarse_kernel, row_valence, row_conduction, row_neighbours, row_weight_index, col_neighbours, col_weight_index, tile_list, weight_table):
    inv_root = 1.0 / math.sqrt(PLANE_WAVES)
    row_rotation = rotation(table_lookup(row_weight_index, weight_table), row_valence, row_conduction)
    groups = jnp.arange(SLAB_ROWS, dtype=jnp.int32) // ROWS_DEVICE
    row_coarse = ((groups[:, None] * GROUP_ROWS + row_neighbours) % COARSE_ROWS).astype(jnp.int32)
    row_mats = jnp.transpose(row_rotation, (0, 2, 1, 3)).reshape(SLAB_ROWS, BAND_PAIRS, CORNERS * BAND_PAIRS)
    kernel_tiles = coarse_kernel.reshape(COARSE_ROWS, BAND_PAIRS, COARSE_COLUMNS, BAND_PAIRS)

    def per_owner(owner_index):
        listed = tile_list[owner_index]
        start = (owner_index * OWNER_COLUMNS).astype(jnp.int32)
        fine_block = lax.dynamic_slice_in_dim(fine_waves, start, OWNER_COLUMNS, 0).astype(jnp.float32)
        neighbours = lax.dynamic_slice_in_dim(col_neighbours, start, OWNER_COLUMNS, 0)
        weight_levels = lax.dynamic_slice_in_dim(col_weight_index, start, OWNER_COLUMNS, 0)
        list_waves = jnp.take(coarse_waves, listed, axis=0)
        valence_terms = []
        conduction_terms = []
        for corner in range(CORNERS):
            paired = jnp.take(list_waves, neighbours[:, corner], axis=0).astype(jnp.float32)
            valence_terms.append(jnp.einsum('fvg,fwg->fvw', fine_block[:, :VALENCE], paired[:, :VALENCE]))
            conduction_terms.append(jnp.einsum('fvg,fwg->fvw', fine_block[:, VALENCE:], paired[:, VALENCE:]))
        valence_correlation = jnp.stack(valence_terms, 1) * inv_root
        conduction_correlation = jnp.stack(conduction_terms, 1) * inv_root
        col_rotation = rotation(table_lookup(weight_levels, weight_table), valence_correlation, conduction_correlation)
        listed_tiles = jnp.take(kernel_tiles, listed, axis=2).reshape(COARSE_ROWS, BAND_PAIRS, LIST_LENGTH * BAND_PAIRS)

        def per_row(row_item):
            rotation_matrix, coarse_rows = row_item
            chosen = jnp.take(listed_tiles, coarse_rows, axis=0).reshape(CORNERS * BAND_PAIRS, LIST_LENGTH * BAND_PAIRS)
            product = jnp.dot(rotation_matrix.astype(jnp.float32), chosen.astype(jnp.float32), preferred_element_type=jnp.float32)
            return product.astype(jnp.bfloat16)
        left_tiles = lax.map(per_row, (row_mats, row_coarse)).reshape(SLAB_ROWS, BAND_PAIRS, LIST_LENGTH, BAND_PAIRS)
        gathered = jnp.take(left_tiles, neighbours, axis=2)
        result = jnp.einsum('rafjb,fjcb->rfac', gathered.astype(jnp.float32), col_rotation.astype(jnp.float32))
        return result.reshape(SLAB_ROWS, OWNER_COLUMNS, BAND_PAIRS * BAND_PAIRS).astype(jnp.bfloat16)
    blocks = lax.map(per_owner, jnp.arange(N_KA, dtype=jnp.int32))
    return jnp.transpose(blocks, (1, 0, 2, 3)).reshape(SLAB_ROWS, FINE_COLUMNS, BAND_PAIRS * BAND_PAIRS)
```

```python
import functools
import math

import jax
import jax.numpy as jnp
from jax import lax
from jax.experimental import pallas as pl
from jax.experimental.pallas import tpu as pltpu
from jax.sharding import PartitionSpec as P

VALENCE = 8
CONDUCTION = 8
BANDS = VALENCE + CONDUCTION
PLANE_WAVES = 40960
CORNERS = 8
BAND_PAIRS = 64
SLOT_COUNT = 4


VMEM = pl.BlockSpec(memory_space=pltpu.VMEM)
SMEM = pl.BlockSpec(memory_space=pltpu.SMEM)
ANY = pl.BlockSpec(memory_space=pl.ANY)


def passed_along(array, axis, by):
    peers = lax.axis_size(axis)
    return lax.ppermute(array, axis, [(i, (i + by) % peers) for i in range(peers)])


def swapped(array, axis, mask):
    peers = lax.axis_size(axis)
    return lax.ppermute(array, axis, [(i, i ^ mask) for i in range(peers)])


def table_lookup(indices, weight_table):
    levels = jnp.arange(weight_table.shape[0], dtype=jnp.int32)
    return jnp.sum(jnp.where(indices[..., None] == levels, weight_table, 0.0), axis=-1)


def pair_tiles(weights, valence_sel, conduction_sel):
    lead = valence_sel.shape[:2]
    outer_product = valence_sel[:, :, :, None, :, None] * conduction_sel[:, :, None, :, None, :]
    outer_product = outer_product.reshape(lead + (BAND_PAIRS, BAND_PAIRS))
    scaled = weights[:, :, None, None] * outer_product / math.sqrt(BAND_PAIRS)
    return scaled.astype(jnp.bfloat16)


def slots_for(list_ref, owner, me, held, slots):
    length = list_ref.shape[1]

    def step(place, carry):
        rank, ids = carry[0], carry[1:]
        column = list_ref[owner, place]
        mine = lax.div(column, held) == me
        ids = tuple(
            jnp.where(jnp.logical_and(mine, rank == slot), column - me * held, ids[slot])
            for slot in range(slots)
        )
        return (rank + jnp.where(mine, 1, 0),) + ids

    zero = jnp.int32(0)
    return lax.fori_loop(0, length, step, (zero,) * (slots + 1), unroll=length <= 8)[1:]


def pack_kernel(peers, me_ref, list_ref, waves_ref, *rest):
    outs, sems = rest[:-1], rest[-1]
    held = waves_ref.shape[0]
    me = me_ref[0]
    copies = []
    for mask in range(1, peers):
        out = outs[mask - 1]
        ids = slots_for(list_ref, lax.bitwise_xor(me, mask), me, held, SLOT_COUNT)
        for slot in range(SLOT_COUNT):
            copy = pltpu.make_async_copy(
                waves_ref.at[ids[slot]], out.at[slot], sems.at[len(copies)]
            )
            copy.start()
            copies.append(copy)
    for copy in copies:
        copy.wait()


def packed_waves(me, tile_list, coarse_waves, peers):
    held, bands, waves = coarse_waves.shape
    block = jax.ShapeDtypeStruct((SLOT_COUNT, bands, waves), coarse_waves.dtype)
    return pl.pallas_call(
        functools.partial(pack_kernel, peers),
        out_shape=[block] * (peers - 1),
        in_specs=[SMEM, SMEM, VMEM],
        out_specs=[ANY] * (peers - 1),
        scratch_shapes=[pltpu.SemaphoreType.DMA(((peers - 1) * SLOT_COUNT,))],
        name="pack",
    )(me, tile_list, coarse_waves)


def rotate_kernel(peers, me_ref, list_ref, near_ref, mats_ref, own_ref, next_ref, *rest):
    outs, chosen = rest[:-1], rest[-1]
    group = own_ref.shape[0]
    held = own_ref.shape[2] // BAND_PAIRS
    me = me_ref[0]
    for corner in range(CORNERS):
        place = near_ref[0, corner]
        rows = pl.ds(corner * BAND_PAIRS, BAND_PAIRS)

        @pl.when(place < group)
        def _():
            chosen[rows, :] = own_ref[place]

        @pl.when(place >= group)
        def _():
            chosen[rows, :] = next_ref[place - group]

    product = jnp.dot(mats_ref[...], chosen[...], preferred_element_type=jnp.float32)
    product = product.astype(jnp.bfloat16)
    tiles = [product[:, p * BAND_PAIRS : (p + 1) * BAND_PAIRS] for p in range(held)]
    for mask in range(peers):
        ids = slots_for(list_ref, lax.bitwise_xor(me, mask), me, held, SLOT_COUNT)
        picked = []
        for slot in range(SLOT_COUNT):
            tile = tiles[0]
            for p in range(1, held):
                tile = jnp.where(ids[slot] == p, tiles[p], tile)
            picked.append(tile)
        outs[mask][...] = jnp.concatenate(picked, axis=1)


def rotated_tiles(me, tile_list, row_neighbours, row_mats, own, upper, peers):
    columns = own.shape[2]
    block = jax.ShapeDtypeStruct((BAND_PAIRS, SLOT_COUNT * BAND_PAIRS), jnp.bfloat16)
    return pl.pallas_call(
        functools.partial(rotate_kernel, peers),
        out_shape=[block] * peers,
        in_specs=[SMEM, SMEM, SMEM, VMEM, VMEM, VMEM],
        out_specs=[VMEM] * peers,
        scratch_shapes=[pltpu.VMEM((CORNERS * BAND_PAIRS, columns), jnp.bfloat16)],
        name="rotate",
    )(me, tile_list, row_neighbours, row_mats, own, upper)


def list_places(list_ref, me, held):
    entries = []
    rank, last = jnp.int32(0), jnp.int32(-1)
    for place in range(list_ref.shape[1]):
        column = list_ref[me, place]
        holder = lax.div(column, held)
        rank = jnp.where(holder == last, rank + 1, 0)
        last = holder
        entries.append((column, lax.bitwise_xor(holder, me), rank))
    return entries


def correlate_kernel(peers, me_ref, list_ref, fine_ref, own_ref, *rest):
    arrived, (out_ref, listed, sems) = rest[: peers - 1], rest[peers - 1 :]
    held = own_ref.shape[0]
    me = me_ref[0]
    fine_count, bands, waves = fine_ref.shape
    length = listed.shape[0]
    for place, (column, mask, rank) in enumerate(list_places(list_ref, me, held)):

        @pl.when(mask == 0)
        def _():
            pltpu.make_async_copy(
                own_ref.at[column - me * held], listed.at[place], sems.at[place]
            ).start()

        for other in range(1, peers):

            @pl.when(mask == other)
            def _():
                pltpu.make_async_copy(
                    arrived[other - 1].at[rank], listed.at[place], sems.at[place]
                ).start()

    for place in range(length):
        pltpu.make_async_copy(own_ref.at[0], listed.at[place], sems.at[place]).wait()
    dense = lax.dot_general(
        fine_ref[...].reshape(fine_count * bands, waves),
        listed[...].reshape(length * bands, waves),
        (((1,), (1,)), ((), ())),
        preferred_element_type=jnp.float32,
    )
    dense = dense.reshape(fine_count, 2, VALENCE, length * bands)
    lanes = lax.broadcasted_iota(jnp.int32, (fine_count, VALENCE, length * bands), 2)
    both = jnp.where(lanes % bands < VALENCE, dense[:, 0], dense[:, 1])
    out_ref[...] = both.reshape(fine_count * VALENCE, length * bands)


def partial_correlations(me, tile_list, fine_waves, coarse_waves, arrived):
    fine_count, bands, waves = fine_waves.shape
    length = tile_list.shape[1]
    peers = len(arrived) + 1
    return pl.pallas_call(
        functools.partial(correlate_kernel, peers),
        out_shape=jax.ShapeDtypeStruct((fine_count * VALENCE, length * bands), jnp.float32),
        in_specs=[SMEM, SMEM, VMEM] + [ANY] * peers,
        out_specs=VMEM,
        scratch_shapes=[
            pltpu.VMEM((length, bands, waves), jnp.bfloat16),
            pltpu.SemaphoreType.DMA((length,)),
        ],
        name="correlate",
    )(me, tile_list, fine_waves, coarse_waves, *arrived)


def finish_kernel(peers, held, me_ref, list_ref, parts_ref, scale_ref, spread_ref, *rest):
    tiles_in, (out_ref, tiles, left, wide, rotation, blocks) = rest[:peers], rest[peers:]
    me = me_ref[0]
    fine_count = out_ref.shape[0]
    length = list_ref.shape[1]
    width = length * BAND_PAIRS
    for mask in range(peers):
        tiles[mask] = tiles_in[mask][...]
    for place, (column, mask, rank) in enumerate(list_places(list_ref, me, held)):
        block = tiles[mask]
        tile = block[:, :BAND_PAIRS]
        for slot in range(1, SLOT_COUNT):
            tile = jnp.where(
                rank == slot, block[:, slot * BAND_PAIRS : (slot + 1) * BAND_PAIRS], tile
            )
        left[:, place * BAND_PAIRS : (place + 1) * BAND_PAIRS] = tile

    total = jnp.sum(parts_ref[...], axis=0) * scale_ref[...]
    high = total.astype(jnp.bfloat16)
    rest1 = total - high.astype(jnp.float32)
    middle = rest1.astype(jnp.bfloat16)
    low = (rest1 - middle.astype(jnp.float32)).astype(jnp.bfloat16)
    spread = spread_ref[...]
    wide[...] = (
        jnp.dot(high, spread, preferred_element_type=jnp.float32)
        + jnp.dot(middle, spread, preferred_element_type=jnp.float32)
    ) + jnp.dot(low, spread, preferred_element_type=jnp.float32)

    for fine in range(fine_count):
        conduction = wide[pl.ds(fine * CONDUCTION, CONDUCTION), width:]
        for v in range(0, VALENCE, 2):
            pair = [
                wide[pl.ds(fine * VALENCE + v + i, 1), :width] * conduction for i in range(2)
            ]
            rotation[pl.ds((fine * VALENCE + v) * CONDUCTION, 2 * CONDUCTION), :] = (
                jnp.concatenate(pair, axis=0).astype(jnp.bfloat16)
            )
    for fine in range(fine_count):
        blocks[pl.ds(fine * BAND_PAIRS, BAND_PAIRS), :] = lax.dot_general(
            left[...],
            rotation[pl.ds(fine * BAND_PAIRS, BAND_PAIRS), :],
            (((1,), (1,)), ((), ())),
            preferred_element_type=jnp.float32,
        )
    for pair in range(0, BAND_PAIRS, 2):
        rows = [blocks[pl.ds(pair + i, fine_count, stride=BAND_PAIRS), :] for i in range(2)]
        out_ref[:, pair * BAND_PAIRS : (pair + 2) * BAND_PAIRS] = jnp.concatenate(
            rows, axis=1
        ).astype(jnp.bfloat16)


def spread_matrix(length):
    rows = jnp.arange(length * BANDS, dtype=jnp.int32)[:, None]
    lanes = jnp.arange(length * BAND_PAIRS, dtype=jnp.int32)[None, :]
    place, w, y = lanes // BAND_PAIRS, lanes // CONDUCTION % VALENCE, lanes % CONDUCTION
    valence = rows == place * BANDS + w
    conduction = rows == place * BANDS + VALENCE + y
    return jnp.concatenate([valence, conduction], axis=1).astype(jnp.bfloat16)


def finished(me, tile_list, parts, scale, tiles, held, fine_count):
    length = tile_list.shape[1]
    peers = len(tiles)
    return pl.pallas_call(
        functools.partial(finish_kernel, peers, held),
        out_shape=jax.ShapeDtypeStruct((fine_count, BAND_PAIRS * BAND_PAIRS), jnp.bfloat16),
        in_specs=[SMEM, SMEM] + [VMEM] * (3 + peers),
        out_specs=VMEM,
        scratch_shapes=[
            pltpu.VMEM((peers, BAND_PAIRS, SLOT_COUNT * BAND_PAIRS), jnp.bfloat16),
            pltpu.VMEM((BAND_PAIRS, length * BAND_PAIRS), jnp.bfloat16),
            pltpu.VMEM((fine_count * VALENCE, 2 * length * BAND_PAIRS), jnp.float32),
            pltpu.VMEM((fine_count * BAND_PAIRS, length * BAND_PAIRS), jnp.bfloat16),
            pltpu.VMEM((fine_count * BAND_PAIRS, BAND_PAIRS), jnp.float32),
        ],
        name="finish",
    )(me, tile_list, parts, scale, spread_matrix(length), *tiles)


def body(
    fine_waves,
    coarse_waves,
    coarse_kernel,
    row_valence,
    row_conduction,
    row_neighbours,
    row_weight_index,
    col_neighbours,
    col_weight_index,
    tile_list,
    weight_table,
):
    peers = lax.axis_size("ka")
    me = lax.axis_index("ka").astype(jnp.int32).reshape(1)
    fine_count = fine_waves.shape[0]
    held = coarse_waves.shape[0]
    length = tile_list.shape[1]

    outgoing = packed_waves(me, tile_list, coarse_waves, peers)
    arrived = [swapped(outgoing[mask - 1], "ka", mask) for mask in range(1, peers)]

    row_rotation = pair_tiles(
        table_lookup(row_weight_index, weight_table), row_valence, row_conduction
    )
    row_mats = jnp.transpose(row_rotation, (0, 2, 1, 3)).reshape(
        BAND_PAIRS, CORNERS * BAND_PAIRS
    )
    upper = passed_along(coarse_kernel, "ga", -1)
    tiles = rotated_tiles(me, tile_list, row_neighbours, row_mats, coarse_kernel, upper, peers)
    tiles = [tiles[0]] + [swapped(tiles[mask], "ka", mask) for mask in range(1, peers)]

    places = jnp.arange(length, dtype=jnp.int32)
    col_weight = table_lookup(col_weight_index, weight_table)
    place_weight = jnp.sum(
        jnp.where(col_neighbours[:, :, None] == places, col_weight[:, :, None], 0.0), axis=1
    )
    inv_root = 1.0 / math.sqrt(PLANE_WAVES)
    band = jnp.arange(BANDS, dtype=jnp.int32)
    scale = jnp.where(
        band < VALENCE, inv_root, place_weight[:, :, None] * (inv_root / math.sqrt(BAND_PAIRS))
    )
    scale = jnp.broadcast_to(scale[:, None], (fine_count, VALENCE, length, BANDS))
    scale = scale.reshape(fine_count * VALENCE, length * BANDS)

    partial = partial_correlations(me, tile_list, fine_waves, coarse_waves, arrived)
    parts = lax.all_gather(partial, "ga")
    return finished(me, tile_list, parts, scale, tiles, held, fine_count)[None]


def solution(mesh):
    placed = (
        P("ka", None, "ga"),
        P("ka", None, "ga"),
        P("ga", None, "ka"),
        P("ga", None, None, None),
        P("ga", None, None, None),
        P("ga", None),
        P("ga", None),
        P("ka", None),
        P("ka", None),
        P(),
        P(),
    )
    return jax.shard_map(
        body, mesh=mesh, in_specs=placed, out_specs=P("ga", "ka", None), check_vma=False
    )
```

```python
import functools
import itertools
import math

import jax
import jax.numpy as jnp
import numpy as np
from jax import lax
from jax.experimental import pallas as pl
from jax.experimental.pallas import tpu as pltpu
from jax.sharding import PartitionSpec as P


VALENCE = 8
CONDUCTION = 8
BANDS = VALENCE + CONDUCTION
PLANE_WAVES = 40960
CORNERS = 8
BAND_PAIRS = 64
SLOT_COUNT = 4
HALF = SLOT_COUNT // 2
FAR = (2, 3)


VMEM = pl.BlockSpec(memory_space=pltpu.VMEM)
SMEM = pl.BlockSpec(memory_space=pltpu.SMEM)
ANY = pl.BlockSpec(memory_space=pl.ANY)
LIMIT = pltpu.CompilerParams(vmem_limit_bytes=16 * 2**20)


def passed_along(array, axis, by):
    peers = lax.axis_size(axis)
    return lax.ppermute(array, axis, [(i, (i + by) % peers) for i in range(peers)])


def swapped(array, axis, mask):
    peers = lax.axis_size(axis)
    return lax.ppermute(array, axis, [(i, i ^ mask) for i in range(peers)])


def slots_for(list_ref, owner, me, held, slots):
    length = list_ref.shape[1]

    def step(place, carry):
        rank, ids = carry[0], carry[1:]
        column = list_ref[owner, place]
        mine = lax.div(column, held) == me
        ids = tuple(
            jnp.where(jnp.logical_and(mine, rank == slot), column - me * held, ids[slot])
            for slot in range(slots)
        )
        return (rank + jnp.where(mine, 1, 0),) + ids

    zero = jnp.int32(0)
    return lax.fori_loop(0, length, step, (zero,) * (slots + 1), unroll=length <= 8)[1:]


def later_index(list_ref, held):
    wants, which, crowded = [], [], jnp.int32(0)
    for owner in range(4):
        count = []
        for mask in FAR:
            total = jnp.int32(0)
            for place in range(list_ref.shape[1]):
                holder = lax.div(list_ref[owner, place], held)
                total = total + jnp.where(holder == owner ^ mask, 1, 0)
            count.append(total > HALF)
        wants.append(jnp.where(jnp.logical_or(*count), 1, 0))
        which.append(jnp.where(count[0], 0, jnp.where(count[1], 1, 0)))
        crowded = crowded + jnp.where(jnp.logical_and(*count), 1, 0)
    level = jnp.maximum(wants[0] + wants[1], wants[2] + wants[3])
    codes = []
    for half in (0, 2):
        one = jnp.where(
            wants[half] > 0, which[half], jnp.where(wants[half + 1] > 0, 2 + which[half + 1], 0)
        )
        codes.append(jnp.where(level == 2, which[half] * 2 + which[half + 1], one))
    index = jnp.where(level == 0, 0, 16 * level - 15 + codes[0] * 4 + codes[1])
    return jnp.where(crowded > 0, 33, index)


def later_options():
    def single(half, code):
        return [(2 * half + code // 2, code % 2)]

    def double(half, code):
        return [(2 * half, code // 2), (2 * half + 1, code % 2)]

    options = [[]]
    for chosen in (single, double):
        for low, high in itertools.product(range(4), repeat=2):
            options.append(chosen(0, low) + chosen(1, high))
    return options + [list(itertools.product(range(4), range(2)))]


def pack_kernel(blocks, me_ref, list_ref, waves_ref, *rest):
    outs, index_ref, sems = rest[:-2], rest[-2], rest[-1]
    held = waves_ref.shape[0]
    me = me_ref[0]
    copies = []
    slots = {}
    for (mask, low, high), out in zip(blocks, outs):
        if mask not in slots:
            slots[mask] = slots_for(
                list_ref, lax.bitwise_xor(me, mask), me, held, SLOT_COUNT
            )
        for slot in range(low, high):
            copy = pltpu.make_async_copy(
                waves_ref.at[slots[mask][slot]], out.at[slot - low], sems.at[len(copies)]
            )
            copy.start()
            copies.append(copy)
    index_ref[0] = later_index(list_ref, held) if list_ref.shape[0] == 4 else jnp.int32(0)
    for copy in copies:
        copy.wait()


def packed_waves(me, tile_list, coarse_waves, blocks):
    _, bands, waves = coarse_waves.shape
    shapes = [
        jax.ShapeDtypeStruct((high - low, bands, waves), coarse_waves.dtype)
        for _, low, high in blocks
    ]
    copies = sum(high - low for _, low, high in blocks)
    return pl.pallas_call(
        functools.partial(pack_kernel, blocks),
        out_shape=shapes + [jax.ShapeDtypeStruct((1,), jnp.int32)],
        in_specs=[SMEM, SMEM, VMEM],
        out_specs=[ANY] * len(blocks) + [SMEM],
        scratch_shapes=[pltpu.SemaphoreType.DMA((copies,))],
        name="pack",
    )(me, tile_list, coarse_waves)


def wave_blocks(peers):
    masks = sorted(range(1, peers), reverse=True)
    if peers != 4:
        return [(mask, 0, SLOT_COUNT) for mask in masks], []
    always = [(mask, 0, HALF) for mask in FAR] + [(1, 0, SLOT_COUNT)]
    return always, [(mask, HALF, SLOT_COUNT) for mask in FAR]


def sent_where_needed(index, packed):
    def sending(option, *packed):
        sent = []
        for which, mask in enumerate(FAR):
            pairs = [(o ^ mask, o) for o, at in option if at == which]
            sent.append(lax.ppermute(packed[which], "ka", pairs) if pairs else packed[which])
        return tuple(sent)

    branches = [functools.partial(sending, option) for option in later_options()]
    return lax.switch(index, branches, *packed)


def split_dot(left, right):
    high = left.astype(jnp.bfloat16)
    rest = left - high.astype(jnp.float32)
    middle = rest.astype(jnp.bfloat16)
    low = (rest - middle.astype(jnp.float32)).astype(jnp.bfloat16)
    parts = [jnp.dot(x, right, preferred_element_type=jnp.float32) for x in (high, middle, low)]
    return (parts[0] + parts[1]) + parts[2]


def turned(small):
    count = small.shape[1]
    rows = lax.broadcasted_iota(jnp.int32, (count, count), 0)
    columns = lax.broadcasted_iota(jnp.int32, (count, count), 1)
    unit = (rows == columns).astype(jnp.float32).astype(jnp.bfloat16)
    values = small.astype(jnp.float32).astype(jnp.bfloat16)
    return lax.dot_general(
        unit, values, (((1,), (1,)), ((), ())), preferred_element_type=jnp.float32
    ).astype(jnp.int32)


def rotate_kernel(
    peers,
    me_ref,
    list_ref,
    near_ref,
    level_ref,
    table_ref,
    valence_ref,
    conduction_ref,
    neighbours_ref,
    levels_ref,
    own_ref,
    next_ref,
    *rest,
):
    outs, scale_ref, (chosen, wide, mats) = rest[:peers], rest[peers], rest[peers + 1 :]
    group = own_ref.shape[0]
    held = own_ref.shape[2] // BAND_PAIRS
    me = me_ref[0]
    for corner in range(CORNERS):
        place = near_ref[0, corner]
        rows = pl.ds(corner * BAND_PAIRS, BAND_PAIRS)

        @pl.when(place < group)
        def _():
            chosen[rows, :] = own_ref[place]

        @pl.when(place >= group)
        def _():
            chosen[rows, :] = next_ref[place - group]

    lanes = lax.broadcasted_iota(jnp.int32, (VALENCE, BAND_PAIRS), 1)
    bands = lax.broadcasted_iota(jnp.int32, (VALENCE, BAND_PAIRS), 0)
    by_valence = (lanes // CONDUCTION == bands).astype(jnp.float32).astype(jnp.bfloat16)
    by_conduction = (lanes % CONDUCTION == bands).astype(jnp.float32).astype(jnp.bfloat16)
    rows = CORNERS * VALENCE
    wide[...] = split_dot(valence_ref[0].reshape(rows, VALENCE), by_valence)
    conduction = split_dot(conduction_ref[0].reshape(rows, CONDUCTION), by_conduction)
    norm = 1.0 / math.sqrt(BAND_PAIRS)
    for corner in range(0, CORNERS, 2):
        for v in range(VALENCE):
            pair = []
            for c in (corner, corner + 1):
                outer_product = (
                    wide[pl.ds(c * VALENCE + v, 1), :]
                    * conduction[c * CONDUCTION : (c + 1) * CONDUCTION]
                )
                pair.append(table_ref[level_ref[0, c]] * outer_product * norm)
            mats[
                pl.ds(v * CONDUCTION, CONDUCTION),
                corner * BAND_PAIRS : (corner + 2) * BAND_PAIRS,
            ] = jnp.concatenate(pair, axis=1)

    product = jnp.dot(
        mats[...].astype(jnp.bfloat16), chosen[...], preferred_element_type=jnp.float32
    )
    product = product.astype(jnp.bfloat16)
    tiles = [product[:, p * BAND_PAIRS : (p + 1) * BAND_PAIRS] for p in range(held)]
    for mask in range(peers):
        ids = slots_for(list_ref, lax.bitwise_xor(me, mask), me, held, SLOT_COUNT)
        picked = []
        for slot in range(SLOT_COUNT):
            tile = tiles[0]
            for p in range(1, held):
                tile = jnp.where(ids[slot] == p, tiles[p], tile)
            picked.append(tile)
        outs[mask][...] = jnp.concatenate(picked, axis=1)

    fine_count = neighbours_ref.shape[1]
    width = scale_ref.shape[1]
    neighbours, levels = turned(neighbours_ref[...]), turned(levels_ref[...])
    weights = jnp.zeros(levels.shape, jnp.float32)
    for level in range(table_ref.shape[0]):
        weights = jnp.where(levels == level, table_ref[level], weights)
    lane = lax.broadcasted_iota(jnp.int32, (fine_count, width), 1)
    weight = jnp.zeros((fine_count, width), jnp.float32)
    for corner in range(CORNERS):
        named = neighbours[:, corner : corner + 1] == lane // BANDS
        weight = weight + jnp.where(named, weights[:, corner : corner + 1], 0.0)
    inv_root = 1.0 / math.sqrt(PLANE_WAVES)
    factor = jnp.where(lane % BANDS < VALENCE, inv_root, weight * (inv_root * norm))
    for fine in range(fine_count):
        scale_ref[pl.ds(fine * VALENCE, VALENCE), :] = jnp.broadcast_to(
            factor[fine : fine + 1], (VALENCE, width)
        )


def rotated_tiles(me, tile_list, row_args, col_args, weight_table, own, upper):
    peers, length = tile_list.shape
    near, level, valence, conduction = row_args
    columns = own.shape[2]
    block = jax.ShapeDtypeStruct((BAND_PAIRS, SLOT_COUNT * BAND_PAIRS), jnp.bfloat16)
    scale = jax.ShapeDtypeStruct((col_args[0].shape[1] * VALENCE, length * BANDS), jnp.float32)
    return pl.pallas_call(
        functools.partial(rotate_kernel, peers),
        out_shape=[block] * peers + [scale],
        in_specs=[SMEM] * 5 + [VMEM] * 6,
        out_specs=[VMEM] * (peers + 1),
        scratch_shapes=[
            pltpu.VMEM((CORNERS * BAND_PAIRS, columns), jnp.bfloat16),
            pltpu.VMEM((CORNERS * VALENCE, BAND_PAIRS), jnp.float32),
            pltpu.VMEM((BAND_PAIRS, CORNERS * BAND_PAIRS), jnp.float32),
        ],
        name="rotate",
    )(me, tile_list, near, level, weight_table, valence, conduction, *col_args, own, upper)


def list_places(list_ref, me, held):
    entries = []
    rank, last = jnp.int32(0), jnp.int32(-1)
    for place in range(list_ref.shape[1]):
        column = list_ref[me, place]
        holder = lax.div(column, held)
        rank = jnp.where(holder == last, rank + 1, 0)
        last = holder
        entries.append((column, lax.bitwise_xor(holder, me), rank))
    return entries


def correlate_kernel(blocks, me_ref, list_ref, fine_hbm, own_ref, *rest):
    arrived, (out_ref, fine, listed, sems) = rest[: len(blocks)], rest[len(blocks) :]
    held = own_ref.shape[0]
    me = me_ref[0]
    fine_count, bands, waves = fine_hbm.shape
    length = listed.shape[0]
    parts = sems.shape[0]
    count = fine_count // parts
    copies = []
    for part in range(parts):
        some = pl.ds(part * count, count)
        copies.append(pltpu.make_async_copy(fine_hbm.at[some], fine.at[some], sems.at[part]))
        copies[-1].start()
    for place, (column, mask, rank) in enumerate(list_places(list_ref, me, held)):

        def fetch(source, at, place=place):
            listed[place] = source[at]

        pl.when(mask == 0)(functools.partial(fetch, own_ref, column - me * held))
        for (other, low, high), source in zip(blocks, arrived):
            here = jnp.logical_and(rank >= low, rank < high)
            pl.when(jnp.logical_and(mask == other, here))(
                functools.partial(fetch, source, rank - low)
            )
    for part in range(parts):
        copies[part].wait()
        dense = lax.dot_general(
            fine[part * count : (part + 1) * count].reshape(count * bands, waves),
            listed[...].reshape(length * bands, waves),
            (((1,), (1,)), ((), ())),
            preferred_element_type=jnp.float32,
        )
        dense = dense.reshape(count, 2, VALENCE, length * bands)
        lanes = lax.broadcasted_iota(jnp.int32, (count, VALENCE, length * bands), 2)
        both = jnp.where(lanes % bands < VALENCE, dense[:, 0], dense[:, 1])
        out_ref[pl.ds(part * count * VALENCE, count * VALENCE), :] = both.reshape(
            count * VALENCE, length * bands
        )


def partial_correlations(me, tile_list, fine_waves, coarse_waves, blocks, arrived):
    fine_count, bands, waves = fine_waves.shape
    length = tile_list.shape[1]
    return pl.pallas_call(
        functools.partial(correlate_kernel, blocks),
        out_shape=jax.ShapeDtypeStruct((fine_count * VALENCE, length * bands), jnp.float32),
        in_specs=[SMEM, SMEM, ANY] + [VMEM] * (1 + len(blocks)),
        out_specs=VMEM,
        scratch_shapes=[
            pltpu.VMEM((fine_count, bands, waves), jnp.bfloat16),
            pltpu.VMEM((length, bands, waves), jnp.bfloat16),
            pltpu.SemaphoreType.DMA((2 if fine_count % 2 == 0 else 1,)),
        ],
        compiler_params=LIMIT,
        name="correlate",
    )(
        me,
        tile_list,
        pltpu.with_memory_space_constraint(fine_waves, pltpu.HBM),
        coarse_waves,
        *arrived,
    )


def finish_kernel(peers, held, me_ref, list_ref, parts_ref, scale_ref, spread_ref, *rest):
    tiles_in, (out_ref, tiles, left, wide, rotation, blocks) = rest[:peers], rest[peers:]
    me = me_ref[0]
    fine_count = out_ref.shape[0]
    length = list_ref.shape[1]
    width = length * BAND_PAIRS
    for mask in range(peers):
        tiles[mask] = tiles_in[mask][...]
    for place, (column, mask, rank) in enumerate(list_places(list_ref, me, held)):
        block = tiles[mask]
        tile = block[:, :BAND_PAIRS]
        for slot in range(1, SLOT_COUNT):
            tile = jnp.where(
                rank == slot, block[:, slot * BAND_PAIRS : (slot + 1) * BAND_PAIRS], tile
            )
        left[:, place * BAND_PAIRS : (place + 1) * BAND_PAIRS] = tile

    total = jnp.sum(parts_ref[...], axis=0) * scale_ref[...]
    wide[...] = split_dot(total, spread_ref[...])

    for fine in range(fine_count):
        conduction = wide[pl.ds(fine * CONDUCTION, CONDUCTION), width:]
        for v in range(0, VALENCE, 2):
            pair = [
                wide[pl.ds(fine * VALENCE + v + i, 1), :width] * conduction for i in range(2)
            ]
            rotation[pl.ds((fine * VALENCE + v) * CONDUCTION, 2 * CONDUCTION), :] = (
                jnp.concatenate(pair, axis=0).astype(jnp.bfloat16)
            )
    for fine in range(fine_count):
        blocks[pl.ds(fine * BAND_PAIRS, BAND_PAIRS), :] = lax.dot_general(
            left[...],
            rotation[pl.ds(fine * BAND_PAIRS, BAND_PAIRS), :],
            (((1,), (1,)), ((), ())),
            preferred_element_type=jnp.float32,
        )
    for pair in range(0, BAND_PAIRS, 2):
        rows = [blocks[pl.ds(pair + i, fine_count, stride=BAND_PAIRS), :] for i in range(2)]
        out_ref[:, pair * BAND_PAIRS : (pair + 2) * BAND_PAIRS] = jnp.concatenate(
            rows, axis=1
        ).astype(jnp.bfloat16)


def spread_matrix(length):
    rows = np.arange(length * BANDS)[:, None]
    lanes = np.arange(length * BAND_PAIRS)[None, :]
    place, w, y = lanes // BAND_PAIRS, lanes // CONDUCTION % VALENCE, lanes % CONDUCTION
    valence = rows == place * BANDS + w
    conduction = rows == place * BANDS + VALENCE + y
    return jnp.asarray(np.concatenate([valence, conduction], axis=1), dtype=jnp.bfloat16)


def finished(me, tile_list, parts, scale, tiles, held, fine_count):
    length = tile_list.shape[1]
    peers = len(tiles)
    return pl.pallas_call(
        functools.partial(finish_kernel, peers, held),
        out_shape=jax.ShapeDtypeStruct((fine_count, BAND_PAIRS * BAND_PAIRS), jnp.bfloat16),
        in_specs=[SMEM, SMEM] + [VMEM] * (3 + peers),
        out_specs=VMEM,
        scratch_shapes=[
            pltpu.VMEM((peers, BAND_PAIRS, SLOT_COUNT * BAND_PAIRS), jnp.bfloat16),
            pltpu.VMEM((BAND_PAIRS, length * BAND_PAIRS), jnp.bfloat16),
            pltpu.VMEM((fine_count * VALENCE, 2 * length * BAND_PAIRS), jnp.float32),
            pltpu.VMEM((fine_count * BAND_PAIRS, length * BAND_PAIRS), jnp.bfloat16),
            pltpu.VMEM((fine_count * BAND_PAIRS, BAND_PAIRS), jnp.float32),
        ],
        compiler_params=LIMIT,
        name="finish",
    )(me, tile_list, parts, scale, spread_matrix(length), *tiles)


def body(
    fine_waves,
    coarse_waves,
    coarse_kernel,
    row_valence,
    row_conduction,
    row_neighbours,
    row_weight_index,
    col_neighbours,
    col_weight_index,
    tile_list,
    weight_table,
):
    peers = lax.axis_size("ka")
    me = lax.axis_index("ka").astype(jnp.int32).reshape(1)
    fine_count = fine_waves.shape[0]
    held = coarse_waves.shape[0]

    always, needed = wave_blocks(peers)
    *packed, index = packed_waves(me, tile_list, coarse_waves, always + needed)
    arrived = []
    for block, (mask, _, _) in zip(packed, always):
        arrived.append(swapped(block, "ka", mask))

    own, _ = lax.optimization_barrier((coarse_kernel, packed[0]))
    upper = passed_along(own, "ga", -1)
    *tiles, scale = rotated_tiles(
        me,
        tile_list,
        (row_neighbours, row_weight_index, row_valence, row_conduction),
        (col_neighbours.T, col_weight_index.T),
        weight_table,
        own,
        upper,
    )
    if needed:
        index, tiles = lax.optimization_barrier((index[0], tiles))
        arrived += sent_where_needed(index, packed[len(always) :])
    tiles = [tiles[0]] + [swapped(tiles[mask], "ka", mask) for mask in range(1, peers)]
    partial = partial_correlations(
        me, tile_list, fine_waves, coarse_waves, always + needed, arrived
    )
    parts = lax.all_gather(partial, "ga")
    return finished(me, tile_list, parts, scale, tiles, held, fine_count)[None]


def solution(mesh):
    placed = (
        P("ka", None, "ga"),
        P("ka", None, "ga"),
        P("ga", None, "ka"),
        P("ga", None, None, None),
        P("ga", None, None, None),
        P("ga", None),
        P("ga", None),
        P("ka", None),
        P("ka", None),
        P(),
        P(),
    )
    return jax.shard_map(
        body, mesh=mesh, in_specs=placed, out_specs=P("ga", "ka", None), check_vma=False
    )
```

```python
import functools
import itertools
import math

import jax
import jax.numpy as jnp
import numpy as np
from jax import lax
from jax.experimental import pallas as pl
from jax.experimental.pallas import tpu as pltpu
from jax.sharding import PartitionSpec as P


VALENCE = 8
CONDUCTION = 8
BANDS = VALENCE + CONDUCTION
PLANE_WAVES = 40960
CORNERS = 8
BAND_PAIRS = 64
SLOT_COUNT = 4
HALF = SLOT_COUNT // 2
FAR = (2, 3)


VMEM = pl.BlockSpec(memory_space=pltpu.VMEM)
SMEM = pl.BlockSpec(memory_space=pltpu.SMEM)
ANY = pl.BlockSpec(memory_space=pl.ANY)
LIMIT = pltpu.CompilerParams(vmem_limit_bytes=16 * 2**20)


def passed_along(array, axis, by):
    peers = lax.axis_size(axis)
    return lax.ppermute(array, axis, [(i, (i + by) % peers) for i in range(peers)])


def swapped(array, axis, mask):
    peers = lax.axis_size(axis)
    return lax.ppermute(array, axis, [(i, i ^ mask) for i in range(peers)])


def slots_for(list_ref, owner, me, held, slots):
    length = list_ref.shape[1]

    def step(place, carry):
        rank, ids = carry[0], carry[1:]
        column = list_ref[owner, place]
        mine = lax.div(column, held) == me
        ids = tuple(
            jnp.where(jnp.logical_and(mine, rank == slot), column - me * held, ids[slot])
            for slot in range(slots)
        )
        return (rank + jnp.where(mine, 1, 0),) + ids

    zero = jnp.int32(0)
    return lax.fori_loop(0, length, step, (zero,) * (slots + 1), unroll=length <= 8)[1:]


def later_index(list_ref, held):
    wants, which, crowded = [], [], jnp.int32(0)
    for owner in range(4):
        count = []
        for mask in FAR:
            total = jnp.int32(0)
            for place in range(list_ref.shape[1]):
                holder = lax.div(list_ref[owner, place], held)
                total = total + jnp.where(holder == owner ^ mask, 1, 0)
            count.append(total > HALF)
        wants.append(jnp.where(jnp.logical_or(*count), 1, 0))
        which.append(jnp.where(count[0], 0, jnp.where(count[1], 1, 0)))
        crowded = crowded + jnp.where(jnp.logical_and(*count), 1, 0)
    level = jnp.maximum(wants[0] + wants[1], wants[2] + wants[3])
    codes = []
    for half in (0, 2):
        one = jnp.where(
            wants[half] > 0, which[half], jnp.where(wants[half + 1] > 0, 2 + which[half + 1], 0)
        )
        codes.append(jnp.where(level == 2, which[half] * 2 + which[half + 1], one))
    index = jnp.where(level == 0, 0, 16 * level - 15 + codes[0] * 4 + codes[1])
    return jnp.where(crowded > 0, 33, index)


def later_options():
    def single(half, code):
        return [(2 * half + code // 2, code % 2)]

    def double(half, code):
        return [(2 * half, code // 2), (2 * half + 1, code % 2)]

    options = [[]]
    for chosen in (single, double):
        for low, high in itertools.product(range(4), repeat=2):
            options.append(chosen(0, low) + chosen(1, high))
    return options + [list(itertools.product(range(4), range(2)))]


def pack_kernel(blocks, me_ref, list_ref, waves_ref, *rest):
    outs, rest = rest[: len(blocks)], rest[len(blocks) :]
    *index_ref, buffer, in_sems, out_sems = rest
    held = waves_ref.shape[0]
    me = me_ref[0]
    ins, stores = [], []
    slots = {}
    for (mask, low, high), out in zip(blocks, outs):
        if mask not in slots:
            slots[mask] = slots_for(
                list_ref, lax.bitwise_xor(me, mask), me, held, SLOT_COUNT
            )
        for slot in range(low, high):
            at = len(ins)
            copy = pltpu.make_async_copy(
                waves_ref.at[slots[mask][slot]], buffer.at[at], in_sems.at[at]
            )
            copy.start()
            ins.append(copy)
            stores.append(
                pltpu.make_async_copy(buffer.at[at], out.at[slot - low], out_sems.at[at])
            )
    for ref in index_ref:
        ref[0] = later_index(list_ref, held)
    for copy, store in zip(ins, stores):
        copy.wait()
        store.start()
    for store in stores:
        store.wait()


def packed_waves(me, tile_list, coarse_waves, blocks, with_index):
    _, bands, waves = coarse_waves.shape
    shapes = [
        jax.ShapeDtypeStruct((high - low, bands, waves), coarse_waves.dtype)
        for _, low, high in blocks
    ]
    copies = sum(high - low for _, low, high in blocks)
    index = [jax.ShapeDtypeStruct((1,), jnp.int32)] if with_index else []
    return pl.pallas_call(
        functools.partial(pack_kernel, blocks),
        out_shape=shapes + index,
        in_specs=[SMEM, SMEM, ANY],
        out_specs=[ANY] * len(blocks) + [SMEM] * len(index),
        scratch_shapes=[
            pltpu.VMEM((copies, bands, waves), coarse_waves.dtype),
            pltpu.SemaphoreType.DMA((copies,)),
            pltpu.SemaphoreType.DMA((copies,)),
        ],
        name="pack",
    )(me, tile_list, coarse_waves)


def wave_blocks(peers):
    masks = sorted(range(1, peers), reverse=True)
    if peers != 4:
        return [(mask, 0, SLOT_COUNT) for mask in masks], []
    always = [(mask, 0, HALF) for mask in FAR] + [(1, 0, SLOT_COUNT)]
    return always, [(mask, HALF, SLOT_COUNT) for mask in FAR]


def sent_where_needed(index, packed):
    def sending(option, *packed):
        sent = []
        for which, mask in enumerate(FAR):
            pairs = [(o ^ mask, o) for o, at in option if at == which]
            sent.append(lax.ppermute(packed[which], "ka", pairs) if pairs else packed[which])
        return tuple(sent)

    branches = [functools.partial(sending, option) for option in later_options()]
    return lax.switch(index, branches, *packed)


def split_dot(left, right):
    high = left.astype(jnp.bfloat16)
    rest = left - high.astype(jnp.float32)
    middle = rest.astype(jnp.bfloat16)
    low = (rest - middle.astype(jnp.float32)).astype(jnp.bfloat16)
    parts = [jnp.dot(x, right, preferred_element_type=jnp.float32) for x in (high, middle, low)]
    return (parts[0] + parts[1]) + parts[2]


def turned(small):
    count = small.shape[1]
    rows = lax.broadcasted_iota(jnp.int32, (count, count), 0)
    columns = lax.broadcasted_iota(jnp.int32, (count, count), 1)
    unit = (rows == columns).astype(jnp.float32).astype(jnp.bfloat16)
    values = small.astype(jnp.float32).astype(jnp.bfloat16)
    return lax.dot_general(
        unit, values, (((1,), (1,)), ((), ())), preferred_element_type=jnp.float32
    ).astype(jnp.int32)


def rotate_kernel(
    peers,
    me_ref,
    list_ref,
    near_ref,
    level_ref,
    table_ref,
    valence_ref,
    conduction_ref,
    neighbours_ref,
    levels_ref,
    own_ref,
    next_ref,
    *rest,
):
    outs, scale_ref, (chosen, wide, mats) = rest[:peers], rest[peers], rest[peers + 1 :]
    group = own_ref.shape[0]
    held = own_ref.shape[2] // BAND_PAIRS
    me = me_ref[0]
    for corner in range(CORNERS):
        place = near_ref[0, corner]
        rows = pl.ds(corner * BAND_PAIRS, BAND_PAIRS)

        @pl.when(place < group)
        def _():
            chosen[rows, :] = own_ref[place]

        @pl.when(place >= group)
        def _():
            chosen[rows, :] = next_ref[place - group]

    lanes = lax.broadcasted_iota(jnp.int32, (VALENCE, BAND_PAIRS), 1)
    bands = lax.broadcasted_iota(jnp.int32, (VALENCE, BAND_PAIRS), 0)
    by_valence = (lanes // CONDUCTION == bands).astype(jnp.float32).astype(jnp.bfloat16)
    by_conduction = (lanes % CONDUCTION == bands).astype(jnp.float32).astype(jnp.bfloat16)
    rows = CORNERS * VALENCE
    wide[...] = split_dot(valence_ref[0].reshape(rows, VALENCE), by_valence)
    conduction = split_dot(conduction_ref[0].reshape(rows, CONDUCTION), by_conduction)
    norm = 1.0 / math.sqrt(BAND_PAIRS)
    for corner in range(0, CORNERS, 2):
        for v in range(VALENCE):
            pair = []
            for c in (corner, corner + 1):
                outer_product = (
                    wide[pl.ds(c * VALENCE + v, 1), :]
                    * conduction[c * CONDUCTION : (c + 1) * CONDUCTION]
                )
                pair.append(table_ref[level_ref[0, c]] * outer_product * norm)
            mats[
                pl.ds(v * CONDUCTION, CONDUCTION),
                corner * BAND_PAIRS : (corner + 2) * BAND_PAIRS,
            ] = jnp.concatenate(pair, axis=1)

    product = jnp.dot(
        mats[...].astype(jnp.bfloat16), chosen[...], preferred_element_type=jnp.float32
    )
    product = product.astype(jnp.bfloat16)
    tiles = [product[:, p * BAND_PAIRS : (p + 1) * BAND_PAIRS] for p in range(held)]
    for mask in range(peers):
        ids = slots_for(list_ref, lax.bitwise_xor(me, mask), me, held, SLOT_COUNT)
        picked = []
        for slot in range(SLOT_COUNT):
            tile = tiles[0]
            for p in range(1, held):
                tile = jnp.where(ids[slot] == p, tiles[p], tile)
            picked.append(tile)
        outs[mask][...] = jnp.concatenate(picked, axis=1)

    fine_count = neighbours_ref.shape[1]
    width = scale_ref.shape[1]
    neighbours, levels = turned(neighbours_ref[...]), turned(levels_ref[...])
    weights = jnp.zeros(levels.shape, jnp.float32)
    for level in range(table_ref.shape[0]):
        weights = jnp.where(levels == level, table_ref[level], weights)
    lane = lax.broadcasted_iota(jnp.int32, (fine_count, width), 1)
    weight = jnp.zeros((fine_count, width), jnp.float32)
    for corner in range(CORNERS):
        named = neighbours[:, corner : corner + 1] == lane // BANDS
        weight = weight + jnp.where(named, weights[:, corner : corner + 1], 0.0)
    inv_root = 1.0 / math.sqrt(PLANE_WAVES)
    factor = jnp.where(lane % BANDS < VALENCE, inv_root, weight * (inv_root * norm))
    for fine in range(fine_count):
        scale_ref[pl.ds(fine * VALENCE, VALENCE), :] = jnp.broadcast_to(
            factor[fine : fine + 1], (VALENCE, width)
        )


def rotated_tiles(me, tile_list, row_args, col_args, weight_table, own, upper):
    peers, length = tile_list.shape
    near, level, valence, conduction = row_args
    columns = own.shape[2]
    block = jax.ShapeDtypeStruct((BAND_PAIRS, SLOT_COUNT * BAND_PAIRS), jnp.bfloat16)
    scale = jax.ShapeDtypeStruct((col_args[0].shape[1] * VALENCE, length * BANDS), jnp.float32)
    return pl.pallas_call(
        functools.partial(rotate_kernel, peers),
        out_shape=[block] * peers + [scale],
        in_specs=[SMEM] * 5 + [VMEM] * 6,
        out_specs=[VMEM] * (peers + 1),
        scratch_shapes=[
            pltpu.VMEM((CORNERS * BAND_PAIRS, columns), jnp.bfloat16),
            pltpu.VMEM((CORNERS * VALENCE, BAND_PAIRS), jnp.float32),
            pltpu.VMEM((BAND_PAIRS, CORNERS * BAND_PAIRS), jnp.float32),
        ],
        name="rotate",
    )(me, tile_list, near, level, weight_table, valence, conduction, *col_args, own, upper)


def list_places(list_ref, me, held):
    entries = []
    rank, last = jnp.int32(0), jnp.int32(-1)
    for place in range(list_ref.shape[1]):
        column = list_ref[me, place]
        holder = lax.div(column, held)
        rank = jnp.where(holder == last, rank + 1, 0)
        last = holder
        entries.append((column, lax.bitwise_xor(holder, me), rank))
    return entries


def correlate_kernel(peers, blocks, me_ref, list_ref, fine_hbm, own_ref, *rest):
    arrived, rest = rest[: len(blocks)], rest[len(blocks) :]
    tiles_in, (out_ref, left_ref, fine, listed, tiles, sem) = rest[:peers], rest[peers:]
    held = own_ref.shape[0]
    me = me_ref[0]
    fine_count, bands, waves = fine_hbm.shape
    length = listed.shape[0]
    copy = pltpu.make_async_copy(fine_hbm, fine, sem)
    copy.start()
    entries = list_places(list_ref, me, held)
    for place, (column, mask, rank) in enumerate(entries):

        def fetch(source, at, place=place):
            listed[place] = source[at]

        pl.when(mask == 0)(functools.partial(fetch, own_ref, column - me * held))
        for (other, low, high), source in zip(blocks, arrived):
            here = jnp.logical_and(rank >= low, rank < high)
            pl.when(jnp.logical_and(mask == other, here))(
                functools.partial(fetch, source, rank - low)
            )
    for mask in range(peers):
        tiles[mask] = tiles_in[mask][...]
    for place, (_, mask, rank) in enumerate(entries):
        block = tiles[mask]
        tile = block[:, :BAND_PAIRS]
        for slot in range(1, SLOT_COUNT):
            tile = jnp.where(
                rank == slot, block[:, slot * BAND_PAIRS : (slot + 1) * BAND_PAIRS], tile
            )
        left_ref[:, place * BAND_PAIRS : (place + 1) * BAND_PAIRS] = tile
    copy.wait()
    dense = lax.dot_general(
        fine[...].reshape(fine_count * bands, waves),
        listed[...].reshape(length * bands, waves),
        (((1,), (1,)), ((), ())),
        preferred_element_type=jnp.float32,
    )
    dense = dense.reshape(fine_count, 2, VALENCE, length * bands)
    lanes = lax.broadcasted_iota(jnp.int32, (fine_count, VALENCE, length * bands), 2)
    both = jnp.where(lanes % bands < VALENCE, dense[:, 0], dense[:, 1])
    out_ref[...] = both.reshape(fine_count * VALENCE, length * bands)


def partial_correlations(me, tile_list, fine_waves, coarse_waves, blocks, arrived, tiles):
    fine_count, bands, waves = fine_waves.shape
    length = tile_list.shape[1]
    peers = len(tiles)
    return pl.pallas_call(
        functools.partial(correlate_kernel, peers, blocks),
        out_shape=[
            jax.ShapeDtypeStruct((fine_count * VALENCE, length * bands), jnp.float32),
            jax.ShapeDtypeStruct((BAND_PAIRS, length * BAND_PAIRS), jnp.bfloat16),
        ],
        in_specs=[SMEM, SMEM, ANY] + [VMEM] * (1 + len(blocks) + peers),
        out_specs=[VMEM, VMEM],
        scratch_shapes=[
            pltpu.VMEM((fine_count, bands, waves), jnp.bfloat16),
            pltpu.VMEM((length, bands, waves), jnp.bfloat16),
            pltpu.VMEM((peers, BAND_PAIRS, SLOT_COUNT * BAND_PAIRS), jnp.bfloat16),
            pltpu.SemaphoreType.DMA(()),
        ],
        compiler_params=LIMIT,
        name="correlate",
    )(
        me,
        tile_list,
        pltpu.with_memory_space_constraint(fine_waves, pltpu.HBM),
        coarse_waves,
        *arrived,
        *tiles,
    )


def finish_kernel(parts_ref, scale_ref, spread_ref, left, out_ref, wide, rotation, blocks):
    fine_count = out_ref.shape[0]
    width = left.shape[1]
    total = jnp.sum(parts_ref[...], axis=0) * scale_ref[...]
    wide[...] = split_dot(total, spread_ref[...])

    for fine in range(fine_count):
        conduction = wide[pl.ds(fine * CONDUCTION, CONDUCTION), width:]
        for v in range(0, VALENCE, 2):
            pair = [
                wide[pl.ds(fine * VALENCE + v + i, 1), :width] * conduction for i in range(2)
            ]
            rotation[pl.ds((fine * VALENCE + v) * CONDUCTION, 2 * CONDUCTION), :] = (
                jnp.concatenate(pair, axis=0).astype(jnp.bfloat16)
            )
    for fine in range(fine_count):
        blocks[pl.ds(fine * BAND_PAIRS, BAND_PAIRS), :] = lax.dot_general(
            left[...],
            rotation[pl.ds(fine * BAND_PAIRS, BAND_PAIRS), :],
            (((1,), (1,)), ((), ())),
            preferred_element_type=jnp.float32,
        )
    for pair in range(0, BAND_PAIRS, 2):
        rows = [blocks[pl.ds(pair + i, fine_count, stride=BAND_PAIRS), :] for i in range(2)]
        out_ref[:, pair * BAND_PAIRS : (pair + 2) * BAND_PAIRS] = jnp.concatenate(
            rows, axis=1
        ).astype(jnp.bfloat16)


def spread_matrix(length):
    rows = np.arange(length * BANDS)[:, None]
    lanes = np.arange(length * BAND_PAIRS)[None, :]
    place, w, y = lanes // BAND_PAIRS, lanes // CONDUCTION % VALENCE, lanes % CONDUCTION
    valence = rows == place * BANDS + w
    conduction = rows == place * BANDS + VALENCE + y
    return jnp.asarray(np.concatenate([valence, conduction], axis=1), dtype=jnp.bfloat16)


def finished(parts, scale, left, fine_count):
    width = left.shape[1]
    return pl.pallas_call(
        finish_kernel,
        out_shape=jax.ShapeDtypeStruct((fine_count, BAND_PAIRS * BAND_PAIRS), jnp.bfloat16),
        in_specs=[VMEM] * 4,
        out_specs=VMEM,
        scratch_shapes=[
            pltpu.VMEM((fine_count * VALENCE, 2 * width), jnp.float32),
            pltpu.VMEM((fine_count * BAND_PAIRS, width), jnp.bfloat16),
            pltpu.VMEM((fine_count * BAND_PAIRS, BAND_PAIRS), jnp.float32),
        ],
        compiler_params=LIMIT,
        name="finish",
    )(parts, scale, spread_matrix(width // BAND_PAIRS), left)


def body(
    fine_waves,
    coarse_waves,
    coarse_kernel,
    row_valence,
    row_conduction,
    row_neighbours,
    row_weight_index,
    col_neighbours,
    col_weight_index,
    tile_list,
    weight_table,
):
    peers = lax.axis_size("ka")
    me = lax.axis_index("ka").astype(jnp.int32).reshape(1)

    always, needed = wave_blocks(peers)
    early = len(FAR) if needed else 1
    packed = packed_waves(me, tile_list, coarse_waves, always[:early], False)
    own, later_list, _ = lax.optimization_barrier((coarse_kernel, tile_list, packed[0]))
    packed += packed_waves(
        me, later_list, coarse_waves, always[early:] + needed, with_index=bool(needed)
    )
    arrived = []
    for place, (mask, _, _) in enumerate(always):
        arrived.append(swapped(packed[place], "ka", mask))

    upper = passed_along(own, "ga", -1)
    *tiles, scale = rotated_tiles(
        me,
        tile_list,
        (row_neighbours, row_weight_index, row_valence, row_conduction),
        (col_neighbours.T, col_weight_index.T),
        weight_table,
        own,
        upper,
    )
    if needed:
        index, tiles = lax.optimization_barrier((packed[-1][0], tiles))
        arrived += sent_where_needed(index, packed[len(always) : -1])
    tiles = [tiles[0]] + [swapped(tiles[mask], "ka", mask) for mask in range(1, peers)]
    partial, left = partial_correlations(
        me, tile_list, fine_waves, coarse_waves, always + needed, arrived, tiles
    )
    parts = lax.all_gather(partial, "ga")
    return finished(parts, scale, left, fine_waves.shape[0])[None]


def solution(mesh):
    placed = (
        P("ka", None, "ga"),
        P("ka", None, "ga"),
        P("ga", None, "ka"),
        P("ga", None, None, None),
        P("ga", None, None, None),
        P("ga", None),
        P("ga", None),
        P("ka", None),
        P("ka", None),
        P(),
        P(),
    )
    return jax.shard_map(
        body, mesh=mesh, in_specs=placed, out_specs=P("ga", "ka", None), check_vma=False
    )
```
